32 devices in a mesh: section: 16 (over z, y, core), walk: 2 (over x).
Axes of the slice: x: 2, y: 2, z: 4, core: 2. Of those that a mesh axis runs over, the one named last changes fastest.
Arguments:
- fields: bfloat16 [16, 8, 800], P('section', None, 'walk'), may hold values from -4 to 4
- cholesky_vectors: bfloat16 [800, 200, 200], P('walk'), may hold values from -0.013 to 0.013
- trial_state: float32 [200, 100], replicated, may hold values from -1.6 to 1.6
- deviation: bfloat16 [16, 8, 200, 100], P('section', 'walk'), may hold values from -0.1796875 to 0.1796875
Outputs:
- density: float32 [8, 200, 200], P('walk')
The draws below stay inside these ranges and needn't reach their ends.
All inputs are finite; a program needn't handle non-finite values.
Results may differ from the reference program's by a relative error of at most 0.0003.
Values sent between devices are 32-bit elements; how exact they have to be, the bound alone decides.
A program may use at most 128 MiB of HBM per device.

```python
import jax
import jax.numpy as jnp
from jax import lax

ORB = 200
ELEC = 100
CHOL = 800
TAYLOR = 6
STEPS = 16
WALKERS = 8


def draw_trial_state(key, part):
    diag_key = jax.random.fold_in(key, 11)
    upper_key = jax.random.fold_in(key, 12)
    lower_key = jax.random.fold_in(key, 13)
    diagonal_part = jax.random.uniform(diag_key, (ELEC,), jnp.float32, 0.8, 1.2)
    upper_noise = 0.3 * jax.random.normal(upper_key, (ELEC, ELEC), jnp.float32) / ELEC ** 0.5
    lower_noise = 0.3 * jax.random.normal(lower_key, (ORB - ELEC, ELEC), jnp.float32) / ORB ** 0.5
    upper_block = jnp.diag(diagonal_part) + upper_noise
    return jnp.clip(jnp.concatenate([upper_block, lower_noise], axis=0), -1.6, 1.6)


def draw_cholesky_vectors(key, part):
    base_key = jax.random.fold_in(key, 21)
    raw_draw = jnp.clip(jax.random.normal(base_key, (CHOL, ORB, ORB), jnp.float32), -4.0, 4.0)
    upper_part = jnp.triu(raw_draw, 1)
    generator = upper_part - jnp.swapaxes(upper_part, 1, 2)
    positions = jnp.arange(ORB)
    occupied = positions < ELEC
    same_block = occupied[:, None] == occupied[None, :]
    inside_scale = 1.8 / (2.0 * ORB * CHOL) ** 0.5
    across_scale = 0.6 / (2.0 * ORB * CHOL * STEPS) ** 0.5
    entry_scale = jnp.where(same_block, inside_scale, across_scale)
    return (generator * entry_scale).astype(jnp.bfloat16)


def block_scale(key, dims, cuts, least, high):
    level, own = 1.0, jax.random.fold_in(key, 6)
    for position, blocks in cuts:
        draws = jnp.exp(jax.random.uniform(jax.random.fold_in(own, position), (blocks,), jnp.float32, least / len(cuts), high / len(cuts)))
        level = level * jnp.repeat(draws, dims[position] // blocks).reshape([-1 if axis == position else 1 for axis in range(len(dims))])
    return level


def normal_values(rng, dims, scale, bound, pieces=(), dtype=jnp.bfloat16):
    values = scale * jax.random.normal(rng, dims, jnp.float32)
    if pieces:
        values = values * block_scale(rng, dims, pieces, -0.22, 0.18)
    return jnp.clip(values, -bound, bound).astype(dtype)


def setup_inputs(seed: int = 0) -> dict:
    keys = jax.random.split(jax.random.key(seed), 5)
    fields = normal_values(keys[0], (STEPS, WALKERS, CHOL), 1.0, 4.0, ((0, 16), (2, 2)))
    cholesky_vectors = draw_cholesky_vectors(jax.random.fold_in(keys[4], 71), 0)
    trial_state = draw_trial_state(jax.random.fold_in(keys[4], 71), 0)
    deviation = normal_values(keys[3], (STEPS, WALKERS, ORB, ELEC), 0.03, 0.1796875, ((0, 16), (1, 2)))
    return dict(fields=fields, cholesky_vectors=cholesky_vectors, trial_state=trial_state, deviation=deviation)


exact_mode = lax.Precision.HIGHEST

def apply_series(field_matrix, left_state):
    series_term = left_state
    summed = left_state
    for degree in range(1, TAYLOR + 1):
        series_term = jnp.einsum('wij,wie->wje', field_matrix, series_term, precision=exact_mode) / degree
        summed = summed + series_term
    return summed

def green_block(left_state, walker):
    intersection = jnp.einsum('wie,wif->wef', left_state, walker, precision=exact_mode)
    solved = jnp.linalg.solve(intersection, jnp.swapaxes(left_state, 1, 2))
    return jnp.einsum('wie,wej->wij', walker, solved, precision=exact_mode)

def reference(fields, cholesky_vectors, trial_state, deviation):
    vector_table = cholesky_vectors.reshape(CHOL, ORB * ORB)
    start_left = jnp.broadcast_to(trial_state, (WALKERS, ORB, ELEC)).astype(jnp.float32)

    def step(state_pair, step_inputs):
        left_state, running = state_pair
        field_row, deviation_row = step_inputs
        field_matrix = jnp.dot(field_row.astype(jnp.float32), vector_table.astype(jnp.float32), preferred_element_type=jnp.float32).reshape(WALKERS, ORB, ORB)
        left_state = apply_series(field_matrix, left_state)
        walker = trial_state + deviation_row.astype(jnp.float32)
        running = running + green_block(left_state, walker)
        return ((left_state, running), None)
    initial = (start_left, jnp.zeros((WALKERS, ORB, ORB), jnp.float32))
    (left_state, running), _ = lax.scan(step, initial, (fields, deviation), reverse=True)
    return running / STEPS
```

```python
import functools
import math

import jax
import jax.numpy as jnp
from jax import lax
from jax.experimental import pallas as pl
from jax.experimental.pallas import tpu as pltpu
from jax.sharding import Mesh, PartitionSpec as P

PACK = 16
SUB = 8


def split(a):
    high = a.astype(jnp.bfloat16)
    return high, (a - high.astype(jnp.float32)).astype(jnp.bfloat16)


def dot_f32(a, b):
    return jnp.dot(a, b, preferred_element_type=jnp.float32)


def dot3(a, b):
    a_high, a_low = split(a)
    b_high, b_low = split(b)
    return dot_f32(a_high, b_high) + (dot_f32(a_high, b_low) + dot_f32(a_low, b_high))


def contract_kernel(orbitals, field_ref, table_ref, out_ref, factor_ref):
    block = pl.program_id(0)
    rows, depth = field_ref.shape[1], field_ref.shape[2]
    low_part = (block * PACK) // orbitals
    high_part = (block * PACK + SUB) // orbitals
    changed = (
        (block == 0)
        | (low_part != ((block - 1) * PACK) // orbitals)
        | (high_part != ((block - 1) * PACK + SUB) // orbitals)
    )

    @pl.when(block == 0)
    def _():
        out_ref[...] = jnp.zeros_like(out_ref)

    @pl.when(changed)
    def _():
        sub = lax.broadcasted_iota(jnp.int32, (PACK, depth), 0)
        lane = lax.broadcasted_iota(jnp.int32, (PACK, depth), 1) % PACK
        for row in range(rows):
            low = field_ref[low_part, pl.ds(row, 1), :]
            high = field_ref[high_part, pl.ds(row, 1), :]
            value = jnp.where(sub < SUB, low, high)
            factor_ref[row * PACK : (row + 1) * PACK, :] = jnp.where(
                sub == lane, value, 0.0
            ).astype(jnp.bfloat16)

    table = table_ref[...].reshape(depth, orbitals)
    product = dot_f32(factor_ref[...], table).reshape(rows, PACK, orbitals)
    bands = orbitals // SUB
    for half in range(PACK // SUB):
        at = pl.multiple_of(((2 * block + half) % bands) * SUB, SUB)
        out_ref[:, pl.ds(at, SUB), :] += product[:, half * SUB : (half + 1) * SUB, :]


def contract(field_rows, cholesky_vectors):
    rows, chol = field_rows.shape
    orbitals = cholesky_vectors.shape[1]
    group = PACK // math.gcd(PACK, orbitals)
    supers = chol // group
    blocks = group * orbitals // PACK
    depth = supers * PACK
    field = field_rows.astype(jnp.float32).reshape(rows, supers, group)
    field = jnp.repeat(jnp.transpose(field, (2, 0, 1)), PACK, axis=2)
    table = cholesky_vectors.reshape(supers, blocks, PACK, orbitals)
    return pl.pallas_call(
        functools.partial(contract_kernel, orbitals),
        grid=(blocks,),
        in_specs=[
            pl.BlockSpec((group, rows, depth), lambda b: (0, 0, 0)),
            pl.BlockSpec((supers, None, PACK, orbitals), lambda b: (0, b, 0, 0)),
        ],
        out_specs=pl.BlockSpec((rows, orbitals, orbitals), lambda b: (0, 0, 0)),
        out_shape=jax.ShapeDtypeStruct((rows, orbitals, orbitals), jnp.float32),
        scratch_shapes=[pltpu.VMEM((rows * PACK, depth), jnp.bfloat16)],
        compiler_params=pltpu.CompilerParams(vmem_limit_bytes=56 * 2**20),
    )(field, table)


def eye(size):
    row = lax.broadcasted_iota(jnp.int32, (size, size), 0)
    column = lax.broadcasted_iota(jnp.int32, (size, size), 1)
    return jnp.where(row == column, 1.0, 0.0)


def series_kernel(place_ref, field_ref, keep_ref, give_ref):
    core = place_ref[1]
    half, orbitals = keep_ref.shape[0], keep_ref.shape[1]
    unit = eye(orbitals)

    def series(v):
        v2 = dot3(v, v)
        v3 = dot3(v2, v)
        upper = unit * (1 / 6) + v * (1 / 24) + v2 * (1 / 120) + v3 * (1 / 720)
        return (unit + v + v2 * 0.5) + dot3(v3, upper)

    for j in range(half):
        keep_ref[j] = series(field_ref[core * half + j])
        give_ref[j] = series(field_ref[(1 - core) * half + j])


def pair_kernel(place_ref, keep_ref, other_ref, out_ref):
    core = place_ref[1]
    for j in range(keep_ref.shape[0]):
        keep, other = keep_ref[j], other_ref[j]
        later = jnp.where(core == 0, other, keep)
        earlier = jnp.where(core == 0, keep, other)
        out_ref[j] = dot3(later, earlier)


def green_kernel(
    scale, place_ref, all_ref, keep_ref, other_ref, trial_ref, walk_ref, walk_other_ref,
    out_ref, left_ref, inter_ref, inverse_ref,
):
    chip, core = place_ref[0], place_ref[1]
    chips, half = all_ref.shape[0], all_ref.shape[1]
    electrons = trial_ref.shape[0]

    for j in range(half):
        left_ref[j] = trial_ref[...]

    def lap(k, _):
        for j in range(half):
            left_ref[j] = dot3(left_ref[j], all_ref[chips - 1 - k, j])
        return 0

    lax.fori_loop(0, chips - 1 - chip, lap, 0)
    unit = eye(electrons)

    def walker(j, step):
        mine = core == step
        return jnp.where(mine, walk_ref[j], walk_other_ref[j])

    for j in range(half):
        keep, other = keep_ref[j], other_ref[j]
        later = jnp.where(core == 0, other, keep)
        earlier = jnp.where(core == 0, keep, other)
        after_late = dot3(left_ref[j], later)
        left_ref[half + j] = after_late
        left_ref[j] = dot3(after_late, earlier)
    for step in range(2):
        for j in range(half):
            at = step * half + j
            inter = dot3(left_ref[at], walker(j, step))
            inter_ref[at] = inter
            flipped = inter.T
            square = dot3(inter, flipped)
            inverse_ref[at] = flipped * lax.rsqrt(jnp.sum(square * square))

    def newton():
        worst = jnp.float32(0.0)
        for at in range(2 * half):
            guess = inverse_ref[at]
            rest = unit - dot3(inter_ref[at], guess)
            inverse_ref[at] = guess + dot3(guess, rest)
            worst = jnp.maximum(worst, jnp.sum(rest * rest))
        return worst

    def going(state):
        return (state[0] < 80) & (state[1] > 1e-4)

    lax.while_loop(going, lambda state: (state[0] + 1, newton()), (jnp.int32(0), jnp.float32(1.0)))
    newton()
    for j in range(half):
        total = None
        for step in range(2):
            at = step * half + j
            green = dot3(walker(j, step), dot3(inverse_ref[at], left_ref[at]))
            total = green if total is None else total + green
        out_ref[j] = total * scale


def call(kernel, out_shapes, args, scratch=()):
    vmem = pl.BlockSpec(memory_space=pltpu.VMEM)
    return pl.pallas_call(
        kernel,
        in_specs=[pl.BlockSpec(memory_space=pltpu.SMEM)] + [vmem] * (len(args) - 1),
        out_specs=jax.tree.map(lambda _: vmem, out_shapes),
        out_shape=out_shapes,
        scratch_shapes=list(scratch),
        compiler_params=pltpu.CompilerParams(vmem_limit_bytes=48 * 2**20),
    )(*args)


def body(fields, cholesky_vectors, trial_state, deviation):
    chol = fields.shape[2]
    orbitals, electrons = trial_state.shape
    per_device = deviation.shape[1]
    half = per_device // 2
    chips = lax.axis_size("chip")
    chip, core = lax.axis_index("chip"), lax.axis_index("core")
    walk_size, walk = lax.axis_size("walk"), lax.axis_index("walk")
    place = jnp.stack([chip, core]).astype(jnp.int32)
    swap = [(0, 1), (1, 0)]

    def half_of(array, which):
        return lax.dynamic_slice_in_dim(array, which * half, half, 0)

    walkers = trial_state + deviation[0].astype(jnp.float32)
    walkers_keep = half_of(walkers, core)
    walkers_other = lax.ppermute(half_of(walkers, 1 - core), "core", swap)

    partial = contract(fields.reshape(-1, chol), cholesky_vectors)

    def owned(device):
        return lax.dynamic_slice_in_dim(partial, device * per_device, per_device, 0)

    field_matrix = owned(walk)
    for shift in range(1, walk_size):
        ring = [(i, (i + shift) % walk_size) for i in range(walk_size)]
        field_matrix = field_matrix + lax.ppermute(
            owned((walk + shift) % walk_size), "walk", ring
        )

    square = jax.ShapeDtypeStruct((half, orbitals, orbitals), jnp.float32)
    keep, give = call(series_kernel, (square, square), (place, field_matrix))
    other = lax.ppermute(give, "core", swap)
    pair = call(pair_kernel, square, (place, keep, other))
    everything = lax.all_gather(pair, "chip")
    density = call(
        functools.partial(green_kernel, 1.0 / (2 * chips)),
        square,
        (place, everything, keep, other, trial_state.T, walkers_keep, walkers_other),
        [
            pltpu.VMEM((2 * half, electrons, orbitals), jnp.float32),
            pltpu.VMEM((2 * half, electrons, electrons), jnp.float32),
            pltpu.VMEM((2 * half, electrons, electrons), jnp.float32),
        ],
    )
    summed = lax.psum(density, "chip")
    return lax.all_gather(summed, "core", axis=0, tiled=True)


def solution(mesh):
    sections, walks = mesh.devices.shape
    split_mesh = Mesh(
        mesh.devices.reshape(sections // 2, 2, walks), ("chip", "core", "walk")
    )
    section = ("chip", "core")
    in_specs = (
        P(section, None, "walk"),
        P("walk", None, None),
        P(),
        P(section, "walk", None, None),
    )
    out_specs = P("walk", None, None)
    return jax.shard_map(
        body, mesh=split_mesh, in_specs=in_specs, out_specs=out_specs, check_vma=False
    )
```

```python
import functools
import math

import jax
import jax.numpy as jnp
from jax import lax
from jax.experimental import pallas as pl
from jax.experimental.pallas import tpu as pltpu
from jax.sharding import Mesh, PartitionSpec as P


PACK = 16
SUB = 8


def split(a):
    high = a.astype(jnp.bfloat16)
    return high, (a - high.astype(jnp.float32)).astype(jnp.bfloat16)


def dot_f32(a, b):
    return jnp.dot(a, b, preferred_element_type=jnp.float32)


def dot3(a, b):
    a_high, a_low = split(a)
    b_high, b_low = split(b)
    return dot_f32(a_high, b_high) + (dot_f32(a_high, b_low) + dot_f32(a_low, b_high))


def contract_kernel(orbitals, field_ref, table_ref, out_ref, factor_ref):
    block = pl.program_id(0)
    rows, depth = field_ref.shape[1], field_ref.shape[2]
    low_part = (block * PACK) // orbitals
    high_part = (block * PACK + SUB) // orbitals
    changed = (
        (block == 0)
        | (low_part != ((block - 1) * PACK) // orbitals)
        | (high_part != ((block - 1) * PACK + SUB) // orbitals)
    )

    @pl.when(block == 0)
    def _():
        out_ref[...] = jnp.zeros_like(out_ref)

    @pl.when(changed)
    def _():
        sub = lax.broadcasted_iota(jnp.int32, (PACK, depth), 0)
        lane = lax.broadcasted_iota(jnp.int32, (PACK, depth), 1) % PACK
        for row in range(rows):
            low = field_ref[low_part, pl.ds(row, 1), :]
            high = field_ref[high_part, pl.ds(row, 1), :]
            value = jnp.where(sub < SUB, low, high)
            factor_ref[row * PACK : (row + 1) * PACK, :] = jnp.where(
                sub == lane, value, 0.0
            ).astype(jnp.bfloat16)

    table = table_ref[...].reshape(depth, orbitals)
    product = dot_f32(factor_ref[...], table).reshape(rows, PACK, orbitals)
    bands = orbitals // SUB
    for half in range(PACK // SUB):
        at = pl.multiple_of(((2 * block + half) % bands) * SUB, SUB)
        out_ref[:, pl.ds(at, SUB), :] += product[:, half * SUB : (half + 1) * SUB, :]


def contract(field_rows, cholesky_vectors):
    rows, chol = field_rows.shape
    orbitals = cholesky_vectors.shape[1]
    group = PACK // math.gcd(PACK, orbitals)
    supers = chol // group
    blocks = group * orbitals // PACK
    depth = supers * PACK
    field = field_rows.astype(jnp.float32).reshape(rows, supers, group)
    field = jnp.repeat(jnp.transpose(field, (2, 0, 1)), PACK, axis=2)
    table = cholesky_vectors.reshape(supers, blocks, PACK, orbitals)
    return pl.pallas_call(
        functools.partial(contract_kernel, orbitals),
        grid=(blocks,),
        in_specs=[
            pl.BlockSpec((group, rows, depth), lambda b: (0, 0, 0)),
            pl.BlockSpec((supers, None, PACK, orbitals), lambda b: (0, b, 0, 0)),
        ],
        out_specs=pl.BlockSpec((rows, orbitals, orbitals), lambda b: (0, 0, 0)),
        out_shape=jax.ShapeDtypeStruct((rows, orbitals, orbitals), jnp.float32),
        scratch_shapes=[pltpu.VMEM((rows * PACK, depth), jnp.bfloat16)],
        compiler_params=pltpu.CompilerParams(vmem_limit_bytes=56 * 2**20),
    )(field, table)


def eye(size):
    row = lax.broadcasted_iota(jnp.int32, (size, size), 0)
    column = lax.broadcasted_iota(jnp.int32, (size, size), 1)
    return jnp.where(row == column, 1.0, 0.0)


def series_kernel(field_ref, out_ref):
    unit = eye(field_ref.shape[1])
    for j in range(field_ref.shape[0]):
        v = field_ref[j]
        v2 = dot3(v, v)
        v3 = dot3(v2, v)
        upper = unit * (1 / 6) + v * (1 / 24) + v2 * (1 / 120) + v3 * (1 / 720)
        out_ref[j] = (unit + v + v2 * 0.5) + dot3(v3, upper)


def block_kernel(place_ref, steps_ref, out_ref):
    members = steps_ref.shape[0]
    member = place_ref[0]

    def step(s):
        return steps_ref[lax.rem(member - s + members, members)]

    parts = [step(s) for s in reversed(range(members))]
    while len(parts) > 1:
        paired = [dot3(parts[i], parts[i + 1]) for i in range(0, len(parts) - 1, 2)]
        parts = paired + parts[len(parts) - len(parts) % 2 :]
    out_ref[...] = parts[0]


def hop_kernel(left_ref, map_ref, out_ref):
    out_ref[...] = dot3(left_ref[...], map_ref[...])


def green_kernel(
    scale, place_ref, left_in_ref, steps_ref, walk_ref, out_ref, left_ref, inter_ref, inverse_ref
):
    members = steps_ref.shape[0]
    member = place_ref[0]
    unit = eye(left_in_ref.shape[0])

    def place(s):
        return lax.rem(member - s + members, members)

    left = left_in_ref[...]
    for s in reversed(range(members)):
        left = dot3(left, steps_ref[place(s)])
        left_ref[s] = left
    for s in range(members):
        inter = dot3(left_ref[s], walk_ref[place(s)])
        inter_ref[s] = inter
        flipped = inter.T
        square = dot3(inter, flipped)
        inverse_ref[s] = flipped * lax.rsqrt(jnp.sum(square * square))

    def newton():
        worst = jnp.float32(0.0)
        for s in range(members):
            guess = inverse_ref[s]
            rest = unit - dot3(inter_ref[s], guess)
            inverse_ref[s] = guess + dot3(guess, rest)
            worst = jnp.maximum(worst, jnp.sum(rest * rest))
        return worst

    def going(state):
        return (state[0] < 80) & (state[1] > 1e-4)

    lax.while_loop(going, lambda state: (state[0] + 1, newton()), (jnp.int32(0), jnp.float32(1.0)))
    newton()
    total = None
    for s in range(members):
        green = dot3(walk_ref[place(s)], dot3(inverse_ref[s], left_ref[s]))
        total = green if total is None else total + green
    out_ref[...] = total * scale


def call(kernel, out_shape, args, scratch=(), scalars=0):
    vmem = pl.BlockSpec(memory_space=pltpu.VMEM)
    smem = pl.BlockSpec(memory_space=pltpu.SMEM)
    return pl.pallas_call(
        kernel,
        in_specs=[smem] * scalars + [vmem] * (len(args) - scalars),
        out_specs=vmem,
        out_shape=out_shape,
        scratch_shapes=list(scratch),
        compiler_params=pltpu.CompilerParams(vmem_limit_bytes=48 * 2**20),
    )(*args)


def exchange(array, axis):
    size, position = lax.axis_size(axis), lax.axis_index(axis)
    parts = [lax.dynamic_index_in_dim(array, position, 0, keepdims=True)]
    for shift in range(1, size):
        ring = [(i, (i + shift) % size) for i in range(size)]
        block = lax.dynamic_index_in_dim(array, (position + shift) % size, 0, keepdims=True)
        parts.append(lax.ppermute(block, axis, ring))
    return jnp.concatenate(parts, axis=0)


def total_over(array, axis):
    size = lax.axis_size(axis)
    if size & (size - 1):
        return lax.psum(array, axis)
    distance = 1
    while distance < size:
        array = array + lax.ppermute(array, axis, [(i, i ^ distance) for i in range(size)])
        distance *= 2
    return array


def body(fields, cholesky_vectors, trial_state, deviation):
    chol = fields.shape[2]
    orbitals, electrons = trial_state.shape
    per_device = deviation.shape[1]
    blocks, members = lax.axis_size("block"), lax.axis_size("member")
    block, member = lax.axis_index("block"), lax.axis_index("member")
    walk_size, walk = lax.axis_size("walk"), lax.axis_index("walk")
    place = member.astype(jnp.int32).reshape(1)

    walkers = exchange(trial_state + deviation[0].astype(jnp.float32), "member")
    partial = contract(fields.reshape(-1, chol), cholesky_vectors)

    def owned(device):
        return lax.dynamic_slice_in_dim(partial, device * per_device, per_device, 0)

    field_matrix = owned(walk)
    for shift in range(1, walk_size):
        ring = [(i, (i + shift) % walk_size) for i in range(walk_size)]
        field_matrix = field_matrix + lax.ppermute(
            owned((walk + shift) % walk_size), "walk", ring
        )

    square = jax.ShapeDtypeStruct((orbitals, orbitals), jnp.float32)
    thin = jax.ShapeDtypeStruct((electrons, orbitals), jnp.float32)
    every = jax.ShapeDtypeStruct((per_device, orbitals, orbitals), jnp.float32)
    steps = exchange(call(series_kernel, every, (field_matrix,)), "member")
    block_map = call(block_kernel, square, (place, steps), scalars=1)
    left = trial_state.T
    for k in range(blocks - 1):
        sent = call(hop_kernel, thin, (left, block_map))
        sent = lax.ppermute(sent, "block", [(i, i - 1) for i in range(1, blocks)])
        left = jnp.where(block == blocks - 2 - k, sent, left)
    density = call(
        functools.partial(green_kernel, 1.0 / (members * blocks)),
        square,
        (place, left, steps, walkers),
        [
            pltpu.VMEM((members, electrons, orbitals), jnp.float32),
            pltpu.VMEM((members, electrons, electrons), jnp.float32),
            pltpu.VMEM((members, electrons, electrons), jnp.float32),
        ],
        scalars=1,
    )
    return lax.all_gather(total_over(density, "block"), "member")


def solution(mesh):
    sections, walks = mesh.devices.shape

    def run(fields, cholesky_vectors, trial_state, deviation):
        members = deviation.shape[1] // walks
        split_mesh = Mesh(
            mesh.devices.reshape(sections // members, members, walks),
            ("block", "member", "walk"),
        )
        section = ("block", "member")
        in_specs = (
            P(section, None, "walk"),
            P("walk", None, None),
            P(),
            P(section, "walk", None, None),
        )
        return jax.shard_map(
            body, mesh=split_mesh, in_specs=in_specs, out_specs=P("walk", None, None),
            check_vma=False,
        )(fields, cholesky_vectors, trial_state, deviation)

    return run
```
